8 devices in a mesh: rep: 1 (over z), dp: 8 (over x, y, core).
Axes of the slice: x: 2, y: 2, z: 1, core: 2. Of those that a mesh axis runs over, the one named last changes fastest.
Arguments:
- x: bfloat16 [8, 2048, 1024], P(('rep', 'dp'))
- dy: bfloat16 [8, 2048, 1024], P(('rep', 'dp'))
- wq: bfloat16 [2, 1024, 1024], P(None, 'dp')
- wk: bfloat16 [2, 1024, 1024], P(None, 'dp')
- wv: bfloat16 [2, 1024, 1024], P(None, 'dp')
- wo: bfloat16 [2, 1024, 1024], P(None, 'dp')
- w_gate: bfloat16 [2, 1024, 3072], P(None, 'dp')
- w_up: bfloat16 [2, 1024, 3072], P(None, 'dp')
- w_down: bfloat16 [2, 3072, 1024], P(None, 'dp')
- m_wq: float32 [2, 1024, 1024], P(None, 'dp')
- m_wk: float32 [2, 1024, 1024], P(None, 'dp')
- m_wv: float32 [2, 1024, 1024], P(None, 'dp')
- m_wo: float32 [2, 1024, 1024], P(None, 'dp')
- m_w_gate: float32 [2, 1024, 3072], P(None, 'dp')
- m_w_up: float32 [2, 1024, 3072], P(None, 'dp')
- m_w_down: float32 [2, 3072, 1024], P(None, 'dp')
- v_wq: float32 [2, 1024, 1024], P(None, 'dp')
- v_wk: float32 [2, 1024, 1024], P(None, 'dp')
- v_wv: float32 [2, 1024, 1024], P(None, 'dp')
- v_wo: float32 [2, 1024, 1024], P(None, 'dp')
- v_w_gate: float32 [2, 1024, 3072], P(None, 'dp')
- v_w_up: float32 [2, 1024, 3072], P(None, 'dp')
- v_w_down: float32 [2, 3072, 1024], P(None, 'dp')
Outputs:
- output 1: bfloat16 [2, 1024, 1024], P('rep', 'dp')
- output 2: bfloat16 [2, 1024, 1024], P('rep', 'dp')
- output 3: bfloat16 [2, 1024, 1024], P('rep', 'dp')
- output 4: bfloat16 [2, 1024, 1024], P('rep', 'dp')
- output 5: bfloat16 [2, 1024, 3072], P('rep', 'dp')
- output 6: bfloat16 [2, 1024, 3072], P('rep', 'dp')
- output 7: bfloat16 [2, 3072, 1024], P('rep', 'dp')
- output 8: float32 [2, 1024, 1024], P('rep', 'dp')
- output 9: float32 [2, 1024, 1024], P('rep', 'dp')
- output 10: float32 [2, 1024, 1024], P('rep', 'dp')
- output 11: float32 [2, 1024, 1024], P('rep', 'dp')
- output 12: float32 [2, 1024, 3072], P('rep', 'dp')
- output 13: float32 [2, 1024, 3072], P('rep', 'dp')
- output 14: float32 [2, 3072, 1024], P('rep', 'dp')
- output 15: float32 [2, 1024, 1024], P('rep', 'dp')
- output 16: float32 [2, 1024, 1024], P('rep', 'dp')
- output 17: float32 [2, 1024, 1024], P('rep', 'dp')
- output 18: float32 [2, 1024, 1024], P('rep', 'dp')
- output 19: float32 [2, 1024, 3072], P('rep', 'dp')
- output 20: float32 [2, 1024, 3072], P('rep', 'dp')
- output 21: float32 [2, 3072, 1024], P('rep', 'dp')
All inputs are finite; a program needn't handle non-finite values.
Results may differ from the reference program's by a relative error of at most 0.024.
Values are sent between devices in bfloat16 or wider.
A program may use at most 2 GiB of HBM per device.

```python
import jax
import jax.numpy as jnp
from jax import lax

SEQUENCES = 8
TOKENS = 2048
D = 1024
HEADS = 8
KV_HEADS = 8
HEAD = 128
FF = 3072
LAYERS = 2
THETA = 10000
NAMES = ("wq", "wk", "wv", "wo", "w_gate", "w_up", "w_down")
SHAPES = {
    "wq": (LAYERS, D, HEADS * HEAD),
    "wk": (LAYERS, D, KV_HEADS * HEAD),
    "wv": (LAYERS, D, KV_HEADS * HEAD),
    "wo": (LAYERS, HEADS * HEAD, D),
    "w_gate": (LAYERS, D, FF),
    "w_up": (LAYERS, D, FF),
    "w_down": (LAYERS, FF, D),
}


def bump(key, n, height):
    away = (jnp.arange(n, dtype=jnp.int32) - jax.random.randint(key, (), 0, n, jnp.int32)) % n
    return jnp.where(away < n // 8, height, 1.0)


def together(key, own, strength):
    shared = jax.random.normal(key, own.shape[1:], jnp.float32)
    return (own + strength * shared) * lax.rsqrt(1 + strength * strength)


def setup_inputs(seed: int = 0, part: int = 0) -> dict:
    kx, kdy, ka, kb, kz, kf, kh, kl, *keys = jax.random.split(jax.random.key(seed), 8 + 3 * len(NAMES))
    kx, kdy, ka, kb = (jax.random.fold_in(k, part) for k in (kx, kdy, ka, kb))
    kw, km, kv = (keys[i::3] for i in range(3))
    shape = (SEQUENCES, TOKENS, D)
    much_x, much_dy = jax.random.uniform(kz, (2,), jnp.float32, 0.0, 1.0)
    loud = 2.0 ** jax.random.uniform(jax.random.fold_in(kz, 1), (), jnp.float32, -1.0, 2.0)
    layers = 2.0 ** jax.random.uniform(kl, (LAYERS, 1, 1), jnp.float32, -1.0, 1.0)
    times = {"wq": 1.0, "wk": 1.0, "wv": 2.0, "wo": layers, "w_gate": 1.0, "w_up": bump(kh, FF, 4.0), "w_down": layers}
    x = together(ka, jax.random.normal(kx, shape, jnp.float32), much_x) * bump(kf, D, 4.0)
    dy = together(kb, jax.random.normal(kdy, shape, jnp.float32), much_dy)
    drawn = {"x": x.astype(jnp.bfloat16), "dy": (loud * dy * (SEQUENCES * TOKENS) ** -0.5).astype(jnp.bfloat16)}
    for key, name in zip(kw, NAMES, strict=True):
        drawn[name] = (jax.random.normal(key, SHAPES[name], jnp.float32) * SHAPES[name][1] ** -0.5 * times[name]).astype(jnp.bfloat16)
    for key, name in zip(km, NAMES, strict=True):
        drawn[f"m_{name}"] = 0.1 * jax.random.normal(key, SHAPES[name], jnp.float32)
    for key, name in zip(kv, NAMES, strict=True):
        drawn[f"v_{name}"] = jax.random.uniform(key, SHAPES[name], jnp.float32, 0.02, 0.06)
    return drawn


def matmul(a, w):
    return jnp.dot(a, w, preferred_element_type=jnp.float32).astype(jnp.bfloat16)


def normed(h):
    wide = h.astype(jnp.float32)
    scale = lax.rsqrt(jnp.mean(wide**2, -1, keepdims=True) + 1e-6)
    return (wide * scale).astype(jnp.bfloat16)


def turned(t, theta):
    half = t.shape[-1] // 2
    angle = jnp.arange(t.shape[0], dtype=jnp.float32)[:, None] * theta ** (-jnp.arange(half, dtype=jnp.float32) / half)
    cos, sin = jnp.cos(angle)[:, None], jnp.sin(angle)[:, None]
    a, b = t[..., :half].astype(jnp.float32), t[..., half:].astype(jnp.float32)
    return jnp.concatenate([a * cos - b * sin, b * cos + a * sin], -1).astype(jnp.bfloat16)


def seen_by(q, k, v):
    tokens, kv = q.shape[0], k.shape[1]
    q = q.reshape(tokens, kv, -1, q.shape[-1])
    scores = jnp.einsum("tgsd,ugd->gstu", q.astype(jnp.float32), k.astype(jnp.float32)) * q.shape[-1] ** -0.5
    place = jnp.arange(tokens)
    weights = jax.nn.softmax(jnp.where(place[:, None] >= place, scores, -jnp.inf), -1).astype(jnp.bfloat16)
    return jnp.einsum("gstu,ugd->tgsd", weights.astype(jnp.float32), v.astype(jnp.float32)).astype(jnp.bfloat16).reshape(tokens, -1)


def layer(h, w):
    a = normed(h)
    q, k = (turned(matmul(a, w[name]).reshape(h.shape[0], -1, HEAD), THETA) for name in ("wq", "wk"))
    h = h + matmul(seen_by(q, k, matmul(a, w["wv"]).reshape(h.shape[0], -1, HEAD)), w["wo"])
    b = normed(h)
    gate = jnp.dot(b, w["w_gate"], preferred_element_type=jnp.float32)
    up = jnp.dot(b, w["w_up"], preferred_element_type=jnp.float32)
    return h + matmul((jax.nn.silu(gate) * up).astype(jnp.bfloat16), w["w_down"])


def adamw(w, m, v, g):
    m = 0.9 * m + 0.1 * g
    v = 0.95 * v + 0.05 * g * g
    step = m * lax.rsqrt(v + 1e-8) + 0.1 * w
    return (w - 0.02 * step).astype(jnp.bfloat16), m, v


def clipped(gradients, sum_of_squares, count):
    factor = jnp.minimum(1.0, 0.5 * lax.rsqrt(sum_of_squares / count + 1e-30))
    return [g * factor for g in gradients]


def stack(weights, h):
    return lax.scan(lambda h, w: (layer(h, w), None), h, weights)[0]


def reference(x, dy, wq, wk, wv, wo, w_gate, w_up, w_down, m_wq, m_wk, m_wv, m_wo, m_w_gate, m_w_up, m_w_down, v_wq, v_wk, v_wv, v_wo, v_w_gate, v_w_up, v_w_down):
    weights = dict(zip(NAMES, (wq, wk, wv, wo, w_gate, w_up, w_down), strict=True))

    def take(so_far, sequence):
        h, by_y = sequence
        _, back = jax.vjp(stack, weights, h)
        by_weights, by_h = back(by_y)
        return jax.tree.map(lambda total, term: total + term.astype(jnp.float32), so_far, by_weights), by_h

    none_yet = {name: jnp.zeros(w.shape, jnp.float32) for name, w in weights.items()}
    by_weights, by_x = lax.scan(take, none_yet, (x, dy))
    gradients = [by_weights[name].astype(jnp.bfloat16).astype(jnp.float32) for name in NAMES]
    gradients = clipped(gradients, sum(jnp.sum(g * g) for g in gradients), sum(g.size for g in gradients))
    first = (m_wq, m_wk, m_wv, m_wo, m_w_gate, m_w_up, m_w_down)
    second = (v_wq, v_wk, v_wv, v_wo, v_w_gate, v_w_up, v_w_down)
    new = [adamw(weights[name].astype(jnp.float32), m, v, g) for name, m, v, g in zip(NAMES, first, second, gradients, strict=True)]
    return tuple(one[which] for which in range(3) for one in new)
```

```python
import functools

import jax
import jax.numpy as jnp
from jax import lax
from jax.experimental import pallas as pl
from jax.experimental.pallas import tpu as pltpu
from jax.sharding import PartitionSpec as P

HEAD = 128
THETA = 10000
NEG = -1e30
HIDDEN = 2 * NEG
LOG2E = 1.4426950408889634
MB = 2**20
VMEM = 60 * MB
BF, F32 = jnp.bfloat16, jnp.float32
BQ, HALF = 512, 256
UNIT, D, FF = 128, 1024, 3072


def _dot(a, b, ca, cb):
    return lax.dot_general(a, b, (((ca,), (cb,)), ((), ())), preferred_element_type=F32)


def _call(body, grid, ins, outs, scratch=(), flops=0, moved=0, exps=0, **more):
    return pl.pallas_call(
        body,
        grid_spec=pltpu.PrefetchScalarGridSpec(
            num_scalar_prefetch=0, grid=grid,
            in_specs=[pl.BlockSpec(block, index) for _, block, index in ins],
            out_specs=[pl.BlockSpec(block, index) for _, _, block, index in outs],
            scratch_shapes=list(scratch)),
        out_shape=[jax.ShapeDtypeStruct(shape, dtype) for shape, dtype, _, _ in outs],
        compiler_params=pltpu.CompilerParams(dimension_semantics=("arbitrary",) * len(grid), vmem_limit_bytes=VMEM),
        cost_estimate=pl.CostEstimate(flops=flops, transcendentals=exps, bytes_accessed=moved),
        **more,
    )(*[a for a, _, _ in ins])


def _rows(bm):
    return (bm, D), lambda i, *_: (i, 0)


def _inner(bm):
    return (bm, D), lambda j, i: (i, 0)


def _tile(bm):
    return (bm, D), lambda j, i: (i, j)


def _units(at):
    return (8, UNIT, D), lambda j, *_: (0, at + j, 0)


def _scale(wide):
    return lax.rsqrt(jnp.mean(wide * wide, -1, keepdims=True) + 1e-6)


def _unit(ref, j, n=1):
    return ref[:, j * UNIT : (j + n) * UNIT, :].reshape(n * D, D)


def _turn(x, c, s):
    return x * c + pltpu.roll(x, HEAD // 2, 1) * s


def _turn_back(x, c, s):
    return x * c + pltpu.roll(x * s, HEAD // 2, 1)


def _qkv_body(h_ref, w_ref, c_ref, s_ref, a_ref, q_ref, k_ref, v_ref):
    wide = h_ref[...].astype(F32)
    a = (wide * _scale(wide)).astype(BF)
    a_ref[...] = a
    c, s = c_ref[...], s_ref[...]
    for u, out in enumerate((q_ref, k_ref, v_ref)):
        w = w_ref[:, u * UNIT : (u + 1) * UNIT, :]
        for at in range(0, D, HALF):
            y = _dot(a, w[:, :, at : at + HALF].reshape(D, HALF), 1, 0)
            if u == 2:
                out[:, at : at + HALF] = y.astype(BF)
            else:
                y = y.astype(BF).astype(F32)
                for n in range(0, HALF, HEAD):
                    out[:, at + n : at + n + HEAD] = _turn(y[:, n : n + HEAD], c, s).astype(BF)


def qkv(h, units, at, cos, sin, bm=256):
    t = h.shape[0]
    rows, table = _rows(bm), ((bm, HEAD), lambda i: (i, 0))
    return _call(_qkv_body, (t // bm,),
                 [(h, *rows), (units, (8, (3 * UNIT), D), lambda i: (0, at // 3, 0)), (cos, *table), (sin, *table)],
                 [((t, D), BF, *rows)] * 4, flops=2 * t * D * FF, moved=t * D * 10 + 6 * MB)


def _attend_body(q_ref, k_ref, v_ref, o_ref, lse_ref, top_s, mix_s, *, heads):
    iq = pl.program_id(0)
    scale = HEAD**-0.5
    e = scale * LOG2E
    top_s[...] = jnp.full(top_s.shape, NEG, F32)
    mix_s[...] = jnp.zeros(mix_s.shape, F32)
    ones = jnp.ones((8, BQ), BF)

    def block(j, masked):
        here = pl.ds(j * BQ, BQ)
        scores = [_dot(k_ref[here, i * HEAD : (i + 1) * HEAD], q_ref[:, i * HEAD : (i + 1) * HEAD], 1, 1) for i in range(heads)]
        if masked:
            ok = lax.broadcasted_iota(jnp.int32, (BQ, BQ), 1) >= lax.broadcasted_iota(jnp.int32, (BQ, BQ), 0)
        weights, keeps = [], []
        for i, s in enumerate(scores):
            if masked:
                s = jnp.where(ok, s, HIDDEN)
            old = top_s[i : i + 1, :]
            top = jnp.maximum(old, s.max(axis=0, keepdims=True))
            top_s[i : i + 1, :] = top
            weights.append(jnp.exp2((s - top) * e).astype(BF))
            keeps.append(jnp.exp2((old - top) * e))
        for i, (p, keep) in enumerate(zip(weights, keeps)):
            values = jnp.concatenate([v_ref[here, i * HEAD : (i + 1) * HEAD].T, ones], axis=0)
            mix_s[i] = mix_s[i] * keep + _dot(values, p, 1, 0)

    lax.fori_loop(0, iq, lambda j, _: block(j, False), None)
    block(iq, True)
    for i in range(heads):
        total = mix_s[i, HEAD : HEAD + 1, :]
        o_ref[:, i * HEAD : (i + 1) * HEAD] = (mix_s[i, :HEAD, :] * (1 / total)).T.astype(BF)
        lse_ref[i // 4, i % 4 : i % 4 + 1, :] = top_s[i : i + 1, :] * scale + jnp.log(total)


def attend(q, k, v):
    t, heads = q.shape[0], q.shape[1] // HEAD
    rows, whole = ((BQ, D), lambda i: (i, 0)), ((t, D), lambda i: (0, 0))
    return _call(functools.partial(_attend_body, heads=heads), (t // BQ,),
                 [(q, *rows), (k, *whole), (v, *whole)],
                 [((t, D), BF, *rows), ((heads // 4, 4, t), F32, (heads // 4, 4, BQ), lambda i: (0, 0, i))],
                 [pltpu.VMEM((heads, BQ), F32), pltpu.VMEM((heads, HEAD + 8, BQ), F32)],
                 flops=4 * t * t * D, moved=t * D * 8, exps=heads * t * t // 2)


def _out_body(h_ref, o_ref, w_ref, h1_ref, b_ref):
    new = (h_ref[...].astype(F32) + _dot(o_ref[...], _unit(w_ref, 0), 1, 0).astype(BF).astype(F32)).astype(BF)
    h1_ref[...] = new
    wide = new.astype(F32)
    b_ref[...] = (wide * _scale(wide)).astype(BF)


def out_proj(h, o, units, at, bm=512):
    t = h.shape[0]
    rows = _rows(bm)
    return _call(_out_body, (t // bm,), [(h, *rows), (o, *rows), (units, (8, UNIT, D), lambda i: (0, at, 0))],
                 [((t, D), BF, *rows)] * 2, flops=2 * t * D * D, moved=t * D * 8 + 2 * MB)


def _up_body(b_ref, wg_ref, wu_ref, gate_ref, up_ref, act_ref):
    b = b_ref[...]
    for at in range(0, D, HALF):
        cut = slice(at, at + HALF)
        gate = _dot(b, wg_ref[:, :, cut].reshape(D, HALF), 1, 0)
        up = _dot(b, wu_ref[:, :, cut].reshape(D, HALF), 1, 0)
        gate_ref[:, cut] = gate
        up_ref[:, cut] = up
        act_ref[:, cut] = (gate * jax.nn.sigmoid(gate) * up).astype(BF)


def ffn_up(b, units, gate_at, up_at, bm=D):
    t = b.shape[0]
    tile = _tile(bm)
    return _call(_up_body, (3, t // bm),
                 [(b, *_inner(bm)), (units, *_units(gate_at)),
                  (units, *_units(up_at))],
                 [((t, FF), F32, *tile), ((t, FF), F32, *tile), ((t, FF), BF, *tile)],
                 flops=4 * t * D * FF, moved=t * FF * 12 + 12 * MB, exps=t * FF)


def _down_body(h_ref, act_ref, w_ref, out_ref, acc):
    j = pl.program_id(1)
    new = _dot(act_ref[...], _unit(w_ref, 0), 1, 0)

    @pl.when(j == 0)
    def _():
        acc[...] = new

    @pl.when(j == 1)
    def _():
        acc[...] += new

    @pl.when(j == 2)
    def _():
        out_ref[...] = (h_ref[...].astype(F32) + (acc[...] + new).astype(BF).astype(F32)).astype(BF)


def ffn_down(h1, act, units, at, bm=D):
    t = h1.shape[0]
    rows = _rows(bm)
    return _call(_down_body, (t // bm, 3),
                 [(h1, *rows), (act, (bm, D), lambda i, j: (i, j)), (units, (8, UNIT, D), lambda i, j: (0, at + j, 0))],
                 [((t, D), BF, *rows)], [pltpu.VMEM((bm, D), F32)],
                 flops=2 * t * D * FF, moved=t * D * 10 + 6 * MB)[0]


def _gated(gate, up, d):
    s = jax.nn.sigmoid(gate)
    silu = gate * s
    return silu, (d * up * (s + silu * (1 - s))).astype(BF), (d * silu).astype(BF)


def _mid_body(dy_ref, wd_ref, d_ref):
    d_ref[...] = _dot(dy_ref[...], _unit(wd_ref, 0), 1, 1).astype(BF)


def ffn_mid(dy, units, down_at, bm=D):
    t = dy.shape[0]
    return _call(_mid_body, (3, t // bm), [(dy, *_inner(bm)), (units, *_units(down_at))],
                 [((t, FF), BF, *_tile(bm))], flops=2 * t * D * FF, moved=t * FF * 3 + 6 * MB)[0]


def _last_body(b_ref, d_ref, wg_ref, wu_ref, act_ref, dg_ref, du_ref):
    b = b_ref[...]
    for at in range(0, D, HALF):
        cut = slice(at, at + HALF)
        gate, up = (_dot(b, w_ref[:, :, cut].reshape(D, HALF), 1, 0) for w_ref in (wg_ref, wu_ref))
        silu, dg_ref[:, cut], du_ref[:, cut] = _gated(gate, up, d_ref[:, cut].astype(F32))
        act_ref[:, cut] = (silu * up).astype(BF)


def ffn_last(b, d, units, gate_at, up_at, bm=D):
    t = b.shape[0]
    tile = _tile(bm)
    return _call(_last_body, (3, t // bm),
                 [(b, *_inner(bm)), (d, *tile), (units, *_units(gate_at)),
                  (units, *_units(up_at))],
                 [((t, FF), BF, *tile)] * 3, flops=4 * t * D * FF, moved=t * FF * 10 + 12 * MB, exps=t * FF)


def _act_body(dy_ref, gate_ref, up_ref, wd_ref, dg_ref, du_ref):
    dy = dy_ref[...]
    for at in range(0, D, HALF):
        cut = slice(at, at + HALF)
        d = _dot(dy, wd_ref[at // UNIT : at // UNIT + 2].reshape(HALF, D), 1, 1).astype(BF).astype(F32)
        _, dg_ref[:, cut], du_ref[:, cut] = _gated(gate_ref[:, cut], up_ref[:, cut], d)


def ffn_act_bwd(dy, gate, up, units, down_at, bm=D):
    t = dy.shape[0]
    tile = _tile(bm)
    return _call(_act_body, (3, t // bm),
                 [(dy, *_inner(bm)), (gate, *tile), (up, *tile), (units, *_units(down_at))],
                 [((t, FF), BF, *tile)] * 2, flops=2 * t * D * FF, moved=t * FF * 14 + 6 * MB, exps=t * FF)


def _norm_back(h, d, dh):
    s = _scale(h)
    return dh + (s * d - h * (s * s * s * jnp.mean(h * d, -1, keepdims=True))).astype(BF).astype(F32)


def _in_body(dg_ref, du_ref, wg_ref, wu_ref, wo_ref, h1_ref, dy_ref, dh_ref, do_ref, acc):
    j = pl.program_id(1)
    new = _dot(dg_ref[...], _unit(wg_ref, 0), 1, 1) + _dot(du_ref[...], _unit(wu_ref, 0), 1, 1)

    @pl.when(j == 0)
    def _():
        acc[...] = new

    @pl.when(j == 1)
    def _():
        acc[...] += new

    @pl.when(j == 2)
    def _():
        d = (acc[...] + new).astype(BF).astype(F32)
        dh = _norm_back(h1_ref[...].astype(F32), d, dy_ref[...].astype(F32)).astype(BF)
        dh_ref[...] = dh
        do_ref[...] = _dot(dh, _unit(wo_ref, 0), 1, 1).astype(BF)


def ffn_in_bwd(dg, du, gu_units, gate_at, up_at, o_units, o_at, h1, dy, bm=D):
    t = h1.shape[0]
    tile, rows = ((bm, D), lambda i, j: (i, j)), _rows(bm)
    return _call(_in_body, (t // bm, 3),
                 [(dg, *tile), (du, *tile), (gu_units, (8, UNIT, D), lambda i, j: (0, gate_at + j, 0)),
                  (gu_units, (8, UNIT, D), lambda i, j: (0, up_at + j, 0)), (o_units, (8, UNIT, D), lambda i, j: (0, o_at, 0)),
                  (h1, *rows), (dy, *rows)],
                 [((t, D), BF, *rows)] * 2, [pltpu.VMEM((bm, D), F32)],
                 flops=4 * t * D * FF + 2 * t * D * D, moved=t * FF * 4 + t * D * 8 + 14 * MB)


def _attend_back_body(q_ref, k_ref, v_ref, do_ref, o_ref, lse_ref, cq_ref, sq_ref, ck_ref, sk_ref, dq_ref, dk_ref, dv_ref, dq_s, dk_s, dv_s, *, heads):
    iq = pl.program_id(1)
    scale = HEAD**-0.5
    e = scale * LOG2E

    @pl.when(iq == 0)
    def _():
        dk_s[...] = jnp.zeros_like(dk_s)
        dv_s[...] = jnp.zeros_like(dv_s)

    dq_s[...] = jnp.zeros_like(dq_s)
    cols = [slice(i * HEAD, (i + 1) * HEAD) for i in range(heads)]
    lses = [lse_ref[0, i : i + 1, :] * LOG2E for i in range(heads)]
    deltas = [(do_ref[:, c].astype(F32) * o_ref[:, c].astype(F32)).T.sum(axis=0, keepdims=True) for c in cols]

    def block(first, keys, q0, masked):
        here = pl.ds(first, keys)
        scores = [_dot(k_ref[here, c], q_ref[q0:, c], 1, 1) for c in cols]
        dps = [_dot(v_ref[here, c], do_ref[q0:, c], 1, 1) for c in cols]
        if masked:
            ok = lax.broadcasted_iota(jnp.int32, scores[0].shape, 1) >= lax.broadcasted_iota(jnp.int32, scores[0].shape, 0)
        for i, c in enumerate(cols):
            p = jnp.exp2(scores[i] * e - lses[i][:, q0:])
            if masked:
                p = jnp.where(ok, p, 0.0)
            ds = (p * (dps[i] - deltas[i][:, q0:])).astype(BF)
            dv_s[i, here, :] += _dot(p.astype(BF), do_ref[q0:, c], 1, 0)
            dk_s[i, here, :] += _dot(ds, q_ref[q0:, c], 1, 0)
            dq_s[i, :, q0:] += _dot(k_ref[here, c].T, ds, 1, 0)

    lax.fori_loop(0, iq, lambda j, _: block(j * BQ, BQ, 0, False), None)
    for q0 in range(0, BQ, HALF):
        block(iq * BQ + q0, HALF, q0, True)
    for i, c in enumerate(cols):
        d = (dq_s[i] * scale).T.astype(BF).astype(F32)
        dq_ref[:, c] = _turn_back(d, cq_ref[...], sq_ref[...]).astype(BF)

    @pl.when(iq == pl.num_programs(1) - 1)
    def _():
        for i, c in enumerate(cols):
            d = (dk_s[i] * scale).astype(BF).astype(F32)
            dk_ref[:, c] = _turn_back(d, ck_ref[...], sk_ref[...]).astype(BF)
            dv_ref[:, c] = dv_s[i].astype(BF)


def attend_bwd(q, k, v, do, o, lse, cos, sin, heads=4):
    t = q.shape[0]
    wide = heads * HEAD
    tile, whole = ((BQ, wide), lambda g, i: (i, g)), ((t, wide), lambda g, i: (0, g))
    near, far = ((BQ, HEAD), lambda g, i: (i, 0)), ((t, HEAD), lambda g, i: (0, 0))
    return _call(functools.partial(_attend_back_body, heads=heads), (D // wide, t // BQ),
                 [(q, *tile), (k, *whole), (v, *whole), (do, *tile), (o, *tile), (lse, (1, heads, BQ), lambda g, i: (g, 0, i)),
                  (cos, *near), (sin, *near), (cos, *far), (sin, *far)],
                 [((t, D), BF, *tile), ((t, D), BF, *whole), ((t, D), BF, *whole)],
                 [pltpu.VMEM((heads, HEAD, BQ), F32), pltpu.VMEM((heads, t, HEAD), F32), pltpu.VMEM((heads, t, HEAD), F32)],
                 flops=10 * t * t * D, moved=t * D * 16, exps=8 * t * t // 2)


def _qkv_back_body(dq_ref, dk_ref, dv_ref, w_ref, h_ref, dh_ref, out_ref):
    d = sum(_dot(ref[...], _unit(w_ref, u), 1, 1) for u, ref in enumerate((dq_ref, dk_ref, dv_ref)))
    out_ref[...] = _norm_back(h_ref[...].astype(F32), d.astype(BF).astype(F32), dh_ref[...].astype(F32)).astype(BF)


def qkv_bwd(dq, dk, dv, units, at, h, dh, bm=256):
    t = h.shape[0]
    rows = _rows(bm)
    return _call(_qkv_back_body, (t // bm,),
                 [(dq, *rows), (dk, *rows), (dv, *rows), (units, (8, (3 * UNIT), D), lambda i: (0, at // 3, 0)), (h, *rows), (dh, *rows)],
                 [((t, D), BF, *rows)], flops=2 * t * D * FF, moved=t * D * 12 + 6 * MB)[0]


def _grads_body(*refs, pairs):
    *ins, out_ref, left, right, sems = refs
    u = pl.program_id(0)
    slot = lax.rem(u, 2)

    def copies(n):
        for side, (held, (which, col)) in enumerate(zip((left, right), pairs[n])):
            yield pltpu.make_async_copy(ins[which].at[:, pl.ds(col * D, D)], held.at[n % 2], sems.at[n % 2, side])

    def start(n):
        for copy in copies(n):
            copy.start()

    pl.when(u == 0)(functools.partial(start, 0))
    for n in range(1, len(pairs)):
        pl.when(u == n - 1)(functools.partial(start, n))
    for side, held in enumerate((left, right)):
        pltpu.make_async_copy(ins[0].at[:, pl.ds(0, D)], held.at[slot], sems.at[slot, side]).wait()
    for at in range(0, D, BQ):
        out_ref[:, :, at : at + BQ] = _dot(left[slot], right[slot, :, at : at + BQ], 0, 0).astype(BF).reshape(8, UNIT, BQ)


def weight_grads(pairs):
    arrays, found = [], []
    for pair in pairs:
        found.append([])
        for a, col in pair:
            if not any(a is x for x in arrays):
                arrays.append(a)
            found[-1].append((next(n for n, x in enumerate(arrays) if a is x), col))
    t, n = arrays[0].shape[0], len(pairs)
    return pl.pallas_call(
        functools.partial(_grads_body, pairs=found),
        grid_spec=pltpu.PrefetchScalarGridSpec(
            num_scalar_prefetch=0, grid=(n,),
            in_specs=[pl.BlockSpec(memory_space=pl.ANY)] * len(arrays),
            out_specs=pl.BlockSpec((8, UNIT, D), lambda u: (0, u, 0)),
            scratch_shapes=[pltpu.VMEM((2, t, D), BF), pltpu.VMEM((2, t, D), BF), pltpu.SemaphoreType.DMA((2, 2))]),
        out_shape=jax.ShapeDtypeStruct((8, UNIT * n, D), BF),
        compiler_params=pltpu.CompilerParams(dimension_semantics=("arbitrary",), vmem_limit_bytes=VMEM),
        cost_estimate=pl.CostEstimate(flops=2 * t * D * D * n, transcendentals=0, bytes_accessed=n * t * D * 4),
    )(*arrays)


def _total_body(part_ref, g_ref, total_ref, mine, theirs, send, recv):
    me, n = lax.axis_index("dp"), theirs.shape[0] + 1
    peers = [lax.rem(me + k, n) for k in range(1, n)]
    g = g_ref[...].astype(F32)
    mine[...] = jnp.full(mine.shape, jnp.sum(g * g), F32) + part_ref[0, 0]
    barrier = pltpu.get_barrier_semaphore()
    for peer in peers:
        pl.semaphore_signal(barrier, inc=1, device_id={"dp": peer}, device_id_type=pl.DeviceIdType.MESH)
    pl.semaphore_wait(barrier, n - 1)
    copies = [pltpu.make_async_remote_copy(src_ref=mine, dst_ref=theirs.at[k], send_sem=send.at[k], recv_sem=recv.at[k],
                                           device_id={"dp": peer}, device_id_type=pl.DeviceIdType.MESH) for k, peer in enumerate(peers)]
    for copy in copies:
        copy.start()
    for copy in copies:
        copy.wait()
    total_ref[...] = mine[...] + jnp.sum(theirs[...], axis=0)


def total_squares(part, g, n):
    return pl.pallas_call(
        _total_body,
        in_specs=[pl.BlockSpec(memory_space=pltpu.SMEM), pl.BlockSpec(memory_space=pltpu.VMEM)],
        out_specs=pl.BlockSpec(memory_space=pltpu.VMEM),
        out_shape=jax.ShapeDtypeStruct((8, UNIT), F32),
        scratch_shapes=[pltpu.VMEM((8, UNIT), F32), pltpu.VMEM((n - 1, 8, UNIT), F32), pltpu.SemaphoreType.DMA((n - 1,)),
                        pltpu.SemaphoreType.DMA((n - 1,))],
        compiler_params=pltpu.CompilerParams(collective_id=0, has_side_effects=True),
        cost_estimate=pl.CostEstimate(flops=MB, transcendentals=0, bytes_accessed=g.size * 2),
    )(part.reshape(1, 1), g)[0, 0]


def adamw(w, m, v, g):
    m = 0.9 * m + 0.1 * g
    v = 0.95 * v + 0.05 * g * g
    step = m * lax.rsqrt(v + 1e-8) + 0.1 * w
    return (w - 0.02 * step).astype(BF), m, v


def clipped(gradients, sum_of_squares, count):
    factor = jnp.minimum(1.0, 0.5 * lax.rsqrt(sum_of_squares / count + 1e-30))
    return [g * factor for g in gradients]


def _pack_body(*refs, plan):
    ins, outs = refs[: len(refs) - len(plan)], refs[len(refs) - len(plan) :]
    for out, parts in zip(outs, plan, strict=True):
        row = 0
        for n, wide in parts:
            if wide:
                for j in range(3):
                    for k in range(8):
                        out[row + j * UNIT : row + (j + 1) * UNIT, k * UNIT : (k + 1) * UNIT] = ins[n][0, :, (k * 3 + j) * UNIT : (k * 3 + j + 1) * UNIT]
                row += (3 * UNIT)
            else:
                rows = ins[n].shape[1]
                out[row : row + rows, :] = ins[n][0]
                row += rows


def pack(*groups):
    ins, plan = [], []
    for group in groups:
        plan.append([])
        for w, number in group:
            plan[-1].append((len(ins), w.shape[2] != D))
            ins.append((w, (1, *w.shape[1:]), functools.partial(lambda number, i: (number, 0, 0), number)))
    rows = [sum(w.shape[1] * w.shape[2] for w, _ in group) // D for group in groups]
    return _call(functools.partial(_pack_body, plan=plan), (1,), ins, [((n, D), BF, (n, D), lambda i: (0, 0)) for n in rows],
                 moved=4096 * sum(rows), flops=2**26)


def join_columns(g):
    return jnp.concatenate([g[j * UNIT : (j + 1) * UNIT, k * UNIT : (k + 1) * UNIT] for k in range(8) for j in range(3)], 1)


def solution(mesh):
    def step(x, dy, *arrays):
        weights, m, v = (arrays[i : i + 7] for i in (0, 7, 14))
        wq, wk, wv, wo, wg, wu, wd = weights
        x, dy = x[0], dy[0]
        t = x.shape[0]

        (p1,) = pack([(wq, 0), (wk, 0), (wv, 0)])
        p2, p3, p4 = pack([(wo, 0), (wg, 0), (wu, 0), (wd, 1)], [(wq, 1), (wk, 1), (wv, 1), (wd, 0)], [(wo, 1), (wg, 1), (wu, 1)])
        g1, g2, g3, g4 = (lax.all_gather(p, "dp", axis=0) for p in (p1, p2, p3, p4))

        angle = jnp.arange(t, dtype=F32)[:, None] * THETA ** (-jnp.arange(HEAD // 2, dtype=F32) / (HEAD // 2))
        cos, sin = jnp.cos(angle), jnp.sin(angle)
        cos, sin = jnp.concatenate([cos, cos], 1), jnp.concatenate([-sin, sin], 1)

        def scatter(units, after=None):
            if after is not None:
                units, _ = lax.optimization_barrier((units, after))
            return lax.psum_scatter(units.reshape(-1, D), "dp", scatter_dimension=0, tiled=True)

        a0, q0, k0, v0 = qkv(x, g1, 0, cos, sin)
        o0, lse0 = attend(q0, k0, v0)
        h1, b0 = out_proj(x, o0, g2, 0)
        gate, up, act0 = ffn_up(b0, g2, 1, 4)
        d1, act0 = lax.optimization_barrier((ffn_mid(dy, g2, 7), act0))
        h2 = ffn_down(h1, act0, g3, 3)
        a1, q1, k1, v1 = qkv(h2, g3, 0, cos, sin)
        o1, lse1 = attend(q1, k1, v1)
        h3, b1 = out_proj(h2, o1, g4, 0)
        act1, dg1, du1 = ffn_last(b1, d1, g4, 1, 4)

        def ffn_grads(b, dg, du, act, dh):
            return weight_grads([*(((b, 0), (dg, j)) for j in range(3)), *(((b, 0), (du, j)) for j in range(3)),
                                 *(((act, j), (dh, 0)) for j in range(3))])

        def attention_grads(a, dq, dk, dv, o, dh):
            return weight_grads([((a, 0), (dq, 0)), ((a, 0), (dk, 0)), ((a, 0), (dv, 0)), ((o, 0), (dh, 0))])

        f1, dg1, du1 = lax.optimization_barrier((ffn_grads(b1, dg1, du1, act1, dy), dg1, du1))
        rf1 = scatter(f1)
        dh3, do1 = ffn_in_bwd(dg1, du1, g4, 1, 4, g4, 0, h3, dy)
        dq1, dk1, dv1 = attend_bwd(q1, k1, v1, do1, o1, lse1, cos, sin)
        t1, dq1, dk1, dv1 = lax.optimization_barrier((attention_grads(a1, dq1, dk1, dv1, o1, dh3), dq1, dk1, dv1))
        rt1 = scatter(t1, rf1)
        dh2 = qkv_bwd(dq1, dk1, dv1, g3, 0, h2, dh3)
        dg0, du0 = ffn_act_bwd(dh2, gate, up, g3, 3)
        f0, dg0, du0 = lax.optimization_barrier((ffn_grads(b0, dg0, du0, act0, dh2), dg0, du0))
        rf0 = scatter(f0, rt1)
        dh1, do0 = ffn_in_bwd(dg0, du0, g2, 1, 4, g2, 0, h1, dh2)
        dq0, dk0, dv0 = attend_bwd(q0, k0, v0, do0, o0, lse0, cos, sin)
        rt0 = scatter(attention_grads(a0, dq0, dk0, dv0, o0, dh1), rf0)

        def blocks(f, a):
            return [*jnp.split(a, 4), *map(join_columns, jnp.split(f, 3)[:2]), jnp.split(f, 3)[2]]

        squares = total_squares(sum(jnp.sum(jnp.square(r.astype(F32))) for r in (rf1, rt1, rf0)), rt0, mesh.shape["dp"])
        gradients = [jnp.stack(pair).astype(F32) for pair in zip(blocks(rf0, rt0), blocks(rf1, rt1), strict=True)]
        gradients = clipped(gradients, squares, lax.psum(1, "dp") * sum(g.size for g in gradients))
        new = [adamw(w.astype(F32), m, v, g) for w, m, v, g in zip(weights, m, v, gradients, strict=True)]
        return tuple(one[which] for which in range(3) for one in new)

    states, cut = P(("rep", "dp"), None, None), P(None, "dp", None)
    return jax.shard_map(
        step,
        mesh=mesh,
        in_specs=(states, states) + (cut,) * 21,
        out_specs=(P("rep", "dp", None),) * 21,
        check_vma=False,
    )
```

```python
import functools

import jax
import jax.numpy as jnp
from jax import lax
from jax.experimental import pallas as pl
from jax.experimental.pallas import tpu as pltpu
from jax.sharding import PartitionSpec as P

HEAD = 128
THETA = 10000
NEG = -1e30
HIDDEN = 2 * NEG
LOG2E = 1.4426950408889634
MB = 2**20
VMEM = 60 * MB
BF, F32 = jnp.bfloat16, jnp.float32
BK, HALF = 512, 256
UNIT, D, FF = 128, 1024, 3072


def _dot(a, b, ca, cb):
    return lax.dot_general(a, b, (((ca,), (cb,)), ((), ())), preferred_element_type=F32)


def _call(body, grid, ins, outs, scratch=(), flops=0, moved=0, exps=0, **more):
    return pl.pallas_call(
        body,
        grid_spec=pltpu.PrefetchScalarGridSpec(
            num_scalar_prefetch=0, grid=grid,
            in_specs=[pl.BlockSpec(block, index) for _, block, index in ins],
            out_specs=[pl.BlockSpec(block, index) for _, _, block, index in outs],
            scratch_shapes=list(scratch)),
        out_shape=[jax.ShapeDtypeStruct(shape, dtype) for shape, dtype, _, _ in outs],
        compiler_params=pltpu.CompilerParams(dimension_semantics=("arbitrary",) * len(grid), vmem_limit_bytes=VMEM),
        cost_estimate=pl.CostEstimate(flops=flops, transcendentals=exps, bytes_accessed=moved),
        **more,
    )(*[a for a, _, _ in ins])


def _rows(bm):
    return (bm, D), lambda i, *_: (i, 0)


def _inner(bm):
    return (bm, D), lambda j, i: (i, 0)


def _tile(bm):
    return (bm, D), lambda j, i: (i, j)


def _units(at):
    return (8, UNIT, D), lambda j, *_: (0, at + j, 0)


def _scale(wide):
    return lax.rsqrt(jnp.mean(wide * wide, -1, keepdims=True) + 1e-6)


def _unit(ref, j, n=1):
    return ref[:, j * UNIT : (j + n) * UNIT, :].reshape(n * D, D)


def _turn(x, c, s):
    return x * c + pltpu.roll(x, HEAD // 2, 1) * s


def _turn_back(x, c, s):
    return x * c + pltpu.roll(x * s, HEAD // 2, 1)


def _qkv_body(h_ref, w_ref, c_ref, s_ref, a_ref, q_ref, k_ref, v_ref):
    wide = h_ref[...].astype(F32)
    a = (wide * _scale(wide)).astype(BF)
    a_ref[...] = a
    c, s = c_ref[...], s_ref[...]
    for u, out in enumerate((q_ref, k_ref, v_ref)):
        w = w_ref[:, u * UNIT : (u + 1) * UNIT, :]
        for at in range(0, D, HALF):
            y = _dot(a, w[:, :, at : at + HALF].reshape(D, HALF), 1, 0)
            if u == 2:
                out[:, at : at + HALF] = y.astype(BF)
            else:
                y = y.astype(BF).astype(F32)
                for n in range(0, HALF, HEAD):
                    out[:, at + n : at + n + HEAD] = _turn(y[:, n : n + HEAD], c, s).astype(BF)


def qkv(h, units, at, cos, sin, bm=256):
    t = h.shape[0]
    rows, table = _rows(bm), ((bm, HEAD), lambda i: (i, 0))
    return _call(_qkv_body, (t // bm,),
                 [(h, *rows), (units, (8, (3 * UNIT), D), lambda i: (0, at // 3, 0)), (cos, *table), (sin, *table)],
                 [((t, D), BF, *rows)] * 4, flops=2 * t * D * FF, moved=t * D * 10 + 6 * MB)


def _hide(x, value):
    keys = x.shape[0]
    ok = lax.broadcasted_iota(jnp.int32, (keys, keys), 1) >= lax.broadcasted_iota(jnp.int32, (keys, keys), 0)
    first = jnp.where(ok, x[:, :keys], value)
    return first if keys == x.shape[1] else jnp.concatenate([first, x[:, keys:]], 1)


def _attend_body(q_ref, k_ref, v_ref, o_ref, lse_ref):
    scale = HEAD**-0.5
    e = scale * LOG2E
    top = mix = None
    tokens = q_ref.shape[0]
    for at in range(0, tokens, BK):
        here = slice(at, at + BK)
        s = _hide(_dot(k_ref[here], q_ref[at:], 1, 1), HIDDEN)
        old, top = top, s.max(axis=0, keepdims=True)
        top = top if old is None else jnp.maximum(old, top)
        values = jnp.concatenate([v_ref[here].T, jnp.ones((8, BK), BF)], axis=0)
        new = _dot(values, jnp.exp2((s - top) * e).astype(BF), 1, 0)
        mix = new if old is None else mix * jnp.exp2((old - top) * e) + new
        total = mix[HEAD : HEAD + 1, :BK]
        o_ref[here] = (mix[:HEAD, :BK] * (1 / total)).T.astype(BF)
        lse_ref[0, :, here] = top[:, :BK] * scale + jnp.log(total)
        if at + BK < tokens:
            top, mix = top[:, BK:], mix[:, BK:]


def _head(t):
    return (t, HEAD), lambda i: (0, i)


def _lse(t):
    return (1, 1, t), lambda i: (i, 0, 0)


def attend(q, k, v):
    t, heads = q.shape[0], q.shape[1] // HEAD
    return _call(_attend_body, (heads,), [(x, *_head(t)) for x in (q, k, v)],
                 [((t, D), BF, *_head(t)), ((heads, 1, t), F32, *_lse(t))],
                 flops=4 * t * t * D, moved=t * D * 8, exps=heads * t * t // 2)


def _out_body(h_ref, o_ref, w_ref, h1_ref, b_ref):
    new = (h_ref[...].astype(F32) + _dot(o_ref[...], _unit(w_ref, 0), 1, 0).astype(BF).astype(F32)).astype(BF)
    h1_ref[...] = new
    wide = new.astype(F32)
    b_ref[...] = (wide * _scale(wide)).astype(BF)


def out_proj(h, o, units, at, bm=512):
    t = h.shape[0]
    rows = _rows(bm)
    return _call(_out_body, (t // bm,), [(h, *rows), (o, *rows), (units, (8, UNIT, D), lambda i: (0, at, 0))],
                 [((t, D), BF, *rows)] * 2, flops=2 * t * D * D, moved=t * D * 8 + 2 * MB)


def _up_body(b_ref, wg_ref, wu_ref, gate_ref, up_ref, act_ref):
    b = b_ref[...]
    for at in range(0, D, HALF):
        cut = slice(at, at + HALF)
        gate = _dot(b, wg_ref[:, :, cut].reshape(D, HALF), 1, 0)
        up = _dot(b, wu_ref[:, :, cut].reshape(D, HALF), 1, 0)
        gate_ref[:, cut] = gate
        up_ref[:, cut] = up
        act_ref[:, cut] = (gate * jax.nn.sigmoid(gate) * up).astype(BF)


def ffn_up(b, units, gate_at, up_at, bm=D):
    t = b.shape[0]
    tile = _tile(bm)
    return _call(_up_body, (3, t // bm),
                 [(b, *_inner(bm)), (units, *_units(gate_at)),
                  (units, *_units(up_at))],
                 [((t, FF), F32, *tile), ((t, FF), F32, *tile), ((t, FF), BF, *tile)],
                 flops=4 * t * D * FF, moved=t * FF * 12 + 12 * MB, exps=t * FF)


def _down_body(h_ref, act_ref, w_ref, out_ref):
    w = jnp.concatenate([_unit(w_ref, j) for j in range(3)], 0)
    out_ref[...] = (h_ref[...].astype(F32) + _dot(act_ref[...], w, 1, 0).astype(BF).astype(F32)).astype(BF)


def ffn_down(h1, act, units, at, bm=256):
    t = h1.shape[0]
    return _call(_down_body, (t // bm,), [(h1, *_rows(bm)), (act, (bm, FF), lambda i: (i, 0)), (units, (8, 3 * UNIT, D), lambda i: (0, at // 3, 0))],
                 [((t, D), BF, *_rows(bm))], flops=2 * t * D * FF, moved=t * D * 10 + 6 * MB)[0]


def _gated(gate, up, d):
    s = jax.nn.sigmoid(gate)
    silu = gate * s
    return silu, (d * up * (s + silu * (1 - s))).astype(BF), (d * silu).astype(BF)


def _mid_body(dy_ref, wd_ref, d_ref):
    d_ref[...] = _dot(dy_ref[...], _unit(wd_ref, 0), 1, 1).astype(BF)


def ffn_mid(dy, units, down_at, bm=D):
    t = dy.shape[0]
    return _call(_mid_body, (3, t // bm), [(dy, *_inner(bm)), (units, *_units(down_at))],
                 [((t, FF), BF, *_tile(bm))], flops=2 * t * D * FF, moved=t * FF * 3 + 6 * MB)[0]


def _last_body(b_ref, d_ref, wg_ref, wu_ref, act_ref, dg_ref, du_ref):
    b = b_ref[...]
    for at in range(0, D, HALF):
        cut = slice(at, at + HALF)
        gate, up = (_dot(b, w_ref[:, :, cut].reshape(D, HALF), 1, 0) for w_ref in (wg_ref, wu_ref))
        silu, dg_ref[:, cut], du_ref[:, cut] = _gated(gate, up, d_ref[:, cut].astype(F32))
        act_ref[:, cut] = (silu * up).astype(BF)


def ffn_last(b, d, units, gate_at, up_at, bm=D):
    t = b.shape[0]
    tile = _tile(bm)
    return _call(_last_body, (3, t // bm),
                 [(b, *_inner(bm)), (d, *tile), (units, *_units(gate_at)),
                  (units, *_units(up_at))],
                 [((t, FF), BF, *tile)] * 3, flops=4 * t * D * FF, moved=t * FF * 10 + 12 * MB, exps=t * FF)


def _act_body(dy_ref, gate_ref, up_ref, wd_ref, dg_ref, du_ref):
    dy = dy_ref[...]
    for at in range(0, D, HALF):
        cut = slice(at, at + HALF)
        d = _dot(dy, wd_ref[at // UNIT : at // UNIT + 2].reshape(HALF, D), 1, 1).astype(BF).astype(F32)
        _, dg_ref[:, cut], du_ref[:, cut] = _gated(gate_ref[:, cut], up_ref[:, cut], d)


def ffn_act_bwd(dy, gate, up, units, down_at, bm=D):
    t = dy.shape[0]
    tile = _tile(bm)
    return _call(_act_body, (3, t // bm),
                 [(dy, *_inner(bm)), (gate, *tile), (up, *tile), (units, *_units(down_at))],
                 [((t, FF), BF, *tile)] * 2, flops=2 * t * D * FF, moved=t * FF * 14 + 6 * MB, exps=t * FF)


def _norm_back(h, d, dh):
    s = _scale(h)
    return dh + (s * d - h * (s * s * s * jnp.mean(h * d, -1, keepdims=True))).astype(BF).astype(F32)


def _in_body(dg_ref, du_ref, wg_ref, wu_ref, wo_any, h1_any, dy_any, dh_ref, do_ref, acc, wo, h1, dy, sems, *, at):
    j = pl.program_id(1)
    rows = pl.ds(pl.program_id(0) * acc.shape[0], acc.shape[0])
    late = [pltpu.make_async_copy(src, dst, sems.at[n]) for n, (src, dst) in
            enumerate(((wo_any.at[:, pl.ds(at * UNIT, UNIT)], wo), (h1_any.at[rows], h1), (dy_any.at[rows], dy)))]

    @pl.when(j == 0)
    def _():
        for copy in late:
            copy.start()

    new = _dot(dg_ref[...], _unit(wg_ref, 0), 1, 1) + _dot(du_ref[...], _unit(wu_ref, 0), 1, 1)

    @pl.when(j == 0)
    def _():
        acc[...] = new

    @pl.when(j == 1)
    def _():
        acc[...] += new

    @pl.when(j == 2)
    def _():
        for copy in late:
            copy.wait()
        d = (acc[...] + new).astype(BF).astype(F32)
        dh = _norm_back(h1[...].astype(F32), d, dy[...].astype(F32)).astype(BF)
        dh_ref[...] = dh
        do_ref[...] = _dot(dh, _unit(wo, 0), 1, 1).astype(BF)


def ffn_in_bwd(dg, du, gu_units, gate_at, up_at, o_units, o_at, h1, dy, bm=1024):
    t = h1.shape[0]
    some = [pl.BlockSpec((bm, D), lambda i, j: (i, j))] * 2
    some += [pl.BlockSpec((8, UNIT, D), functools.partial(lambda at, i, j: (0, at + j, 0), at)) for at in (gate_at, up_at)]
    return pl.pallas_call(
        functools.partial(_in_body, at=o_at),
        grid_spec=pltpu.PrefetchScalarGridSpec(
            num_scalar_prefetch=0, grid=(t // bm, FF // D),
            in_specs=some + [pl.BlockSpec(memory_space=pl.ANY)] * 3,
            out_specs=[pl.BlockSpec(*_rows(bm))] * 2,
            scratch_shapes=[pltpu.VMEM((bm, D), F32), pltpu.VMEM((8, UNIT, D), BF), pltpu.VMEM((bm, D), BF), pltpu.VMEM((bm, D), BF),
                            pltpu.SemaphoreType.DMA((3,))]),
        out_shape=[jax.ShapeDtypeStruct((t, D), BF)] * 2,
        compiler_params=pltpu.CompilerParams(dimension_semantics=("arbitrary",) * 2, vmem_limit_bytes=VMEM),
        cost_estimate=pl.CostEstimate(flops=4 * t * D * FF + 2 * t * D * D, transcendentals=0, bytes_accessed=t * FF * 4 + t * D * 8 + 14 * MB),
    )(dg, du, gu_units, gu_units, o_units, h1, dy)


def _attend_back_body(q_ref, k_ref, v_ref, do_ref, o_ref, lse_ref, c_ref, s_ref, dq_ref, dk_ref, dv_ref, dq_s):
    scale = HEAD**-0.5
    c, s = c_ref, s_ref
    lse = lse_ref[0] * LOG2E
    delta = (do_ref[...].astype(F32) * o_ref[...].astype(F32)).T.sum(axis=0, keepdims=True)
    dq_s[...] = jnp.zeros_like(dq_s)
    for at in range(0, q_ref.shape[0], HALF):
        here = slice(at, at + HALF)
        p = _hide(jnp.exp2(_dot(k_ref[here], q_ref[at:], 1, 1) * (scale * LOG2E) - lse[:, at:]), 0.0)
        ds = (p * (_dot(v_ref[here], do_ref[at:], 1, 1) - delta[:, at:])).astype(BF)
        dv_ref[here] = _dot(p.astype(BF), do_ref[at:], 1, 0).astype(BF)
        dk = (_dot(ds, q_ref[at:], 1, 0) * scale).astype(BF).astype(F32)
        dk_ref[here] = _turn_back(dk, c[here], s[here]).astype(BF)
        dq_s[:, at:] += _dot(k_ref[here].T, ds, 1, 0)
    dq_ref[...] = _turn_back((dq_s[...] * scale).T.astype(BF).astype(F32), c[...], s[...]).astype(BF)


def attend_bwd(q, k, v, do, o, lse, cos, sin):
    t, heads = q.shape[0], q.shape[1] // HEAD
    return _call(_attend_back_body, (heads,),
                 [*((x, *_head(t)) for x in (q, k, v, do, o)), (lse, *_lse(t)), *((x, (t, HEAD), lambda i: (0, 0)) for x in (cos, sin))],
                 [((t, D), BF, *_head(t))] * 3, [pltpu.VMEM((HEAD, t), F32)],
                 flops=10 * t * t * D, moved=t * D * 16, exps=heads * t * t // 2)


def _qkv_back_body(dq_ref, dk_ref, dv_ref, w_ref, h_ref, dh_ref, out_ref):
    d = sum(_dot(ref[...], _unit(w_ref, u), 1, 1) for u, ref in enumerate((dq_ref, dk_ref, dv_ref)))
    out_ref[...] = _norm_back(h_ref[...].astype(F32), d.astype(BF).astype(F32), dh_ref[...].astype(F32)).astype(BF)


def qkv_bwd(dq, dk, dv, units, at, h, dh, bm=256):
    t = h.shape[0]
    rows = _rows(bm)
    return _call(_qkv_back_body, (t // bm,),
                 [(dq, *rows), (dk, *rows), (dv, *rows), (units, (8, (3 * UNIT), D), lambda i: (0, at // 3, 0)), (h, *rows), (dh, *rows)],
                 [((t, D), BF, *rows)], flops=2 * t * D * FF, moved=t * D * 12 + 6 * MB)[0]


def _grads_body(*refs, pairs):
    *ins, out_ref, left, right, sems = refs
    u = pl.program_id(0)
    slot = lax.rem(u, 2)

    def copies(n):
        for side, (held, (which, col)) in enumerate(zip((left, right), pairs[n])):
            yield pltpu.make_async_copy(ins[which].at[:, pl.ds(col * D, D)], held.at[n % 2], sems.at[n % 2, side])

    def start(n):
        for copy in copies(n):
            copy.start()

    pl.when(u == 0)(functools.partial(start, 0))
    for n in range(1, len(pairs)):
        pl.when(u == n - 1)(functools.partial(start, n))
    for side, held in enumerate((left, right)):
        pltpu.make_async_copy(ins[0].at[:, pl.ds(0, D)], held.at[slot], sems.at[slot, side]).wait()
    for at in range(0, D, BK):
        out_ref[:, :, at : at + BK] = _dot(left[slot], right[slot, :, at : at + BK], 0, 0).astype(BF).reshape(8, UNIT, BK)


def weight_grads(pairs):
    arrays, found = [], []
    for pair in pairs:
        found.append([])
        for a, col in pair:
            if not any(a is x for x in arrays):
                arrays.append(a)
            found[-1].append((next(n for n, x in enumerate(arrays) if a is x), col))
    t, n = arrays[0].shape[0], len(pairs)
    return pl.pallas_call(
        functools.partial(_grads_body, pairs=found),
        grid_spec=pltpu.PrefetchScalarGridSpec(
            num_scalar_prefetch=0, grid=(n,),
            in_specs=[pl.BlockSpec(memory_space=pl.ANY)] * len(arrays),
            out_specs=pl.BlockSpec((8, UNIT, D), lambda u: (0, u, 0)),
            scratch_shapes=[pltpu.VMEM((2, t, D), BF), pltpu.VMEM((2, t, D), BF), pltpu.SemaphoreType.DMA((2, 2))]),
        out_shape=jax.ShapeDtypeStruct((8, UNIT * n, D), BF),
        compiler_params=pltpu.CompilerParams(dimension_semantics=("arbitrary",), vmem_limit_bytes=VMEM),
        cost_estimate=pl.CostEstimate(flops=2 * t * D * D * n, transcendentals=0, bytes_accessed=n * t * D * 4),
    )(*arrays)


def _total_body(part_ref, g_ref, total_ref, mine, theirs, send, recv):
    me, n = lax.axis_index("dp"), theirs.shape[0] + 1
    peers = [lax.rem(me + k, n) for k in range(1, n)]
    g = g_ref[...].astype(F32)
    mine[...] = jnp.full(mine.shape, jnp.sum(g * g), F32) + part_ref[0, 0]
    barrier = pltpu.get_barrier_semaphore()
    for peer in peers:
        pl.semaphore_signal(barrier, inc=1, device_id={"dp": peer}, device_id_type=pl.DeviceIdType.MESH)
    pl.semaphore_wait(barrier, n - 1)
    copies = [pltpu.make_async_remote_copy(src_ref=mine, dst_ref=theirs.at[k], send_sem=send.at[k], recv_sem=recv.at[k],
                                           device_id={"dp": peer}, device_id_type=pl.DeviceIdType.MESH) for k, peer in enumerate(peers)]
    for copy in copies:
        copy.start()
    for copy in copies:
        copy.wait()
    total_ref[...] = mine[...] + jnp.sum(theirs[...], axis=0)


def total_squares(part, g, n):
    return pl.pallas_call(
        _total_body,
        in_specs=[pl.BlockSpec(memory_space=pltpu.SMEM), pl.BlockSpec(memory_space=pltpu.VMEM)],
        out_specs=pl.BlockSpec(memory_space=pltpu.VMEM),
        out_shape=jax.ShapeDtypeStruct((8, UNIT), F32),
        scratch_shapes=[pltpu.VMEM((8, UNIT), F32), pltpu.VMEM((n - 1, 8, UNIT), F32), pltpu.SemaphoreType.DMA((n - 1,)),
                        pltpu.SemaphoreType.DMA((n - 1,))],
        compiler_params=pltpu.CompilerParams(collective_id=0, has_side_effects=True),
        cost_estimate=pl.CostEstimate(flops=MB, transcendentals=0, bytes_accessed=g.size * 2),
    )(part.reshape(1, 1), g)[0, 0]


def adamw(w, m, v, g):
    m = 0.9 * m + 0.1 * g
    v = 0.95 * v + 0.05 * g * g
    step = m * lax.rsqrt(v + 1e-8) + 0.1 * w
    return (w - 0.02 * step).astype(BF), m, v


def clipped(gradients, sum_of_squares, count):
    factor = jnp.minimum(1.0, 0.5 * lax.rsqrt(sum_of_squares / count + 1e-30))
    return [g * factor for g in gradients]


def _pack_body(*refs, plan):
    ins, outs = refs[: len(refs) - len(plan)], refs[len(refs) - len(plan) :]
    for out, parts in zip(outs, plan, strict=True):
        row = 0
        for n, wide in parts:
            if wide:
                for j in range(3):
                    for k in range(8):
                        out[row + j * UNIT : row + (j + 1) * UNIT, k * UNIT : (k + 1) * UNIT] = ins[n][0, :, (k * 3 + j) * UNIT : (k * 3 + j + 1) * UNIT]
                row += (3 * UNIT)
            else:
                rows = ins[n].shape[1]
                out[row : row + rows, :] = ins[n][0]
                row += rows


def pack(*groups):
    ins, plan = [], []
    for group in groups:
        plan.append([])
        for w, number in group:
            plan[-1].append((len(ins), w.shape[2] != D))
            ins.append((w, (1, *w.shape[1:]), functools.partial(lambda number, i: (number, 0, 0), number)))
    rows = [sum(w.shape[1] * w.shape[2] for w, _ in group) // D for group in groups]
    return _call(functools.partial(_pack_body, plan=plan), (1,), ins, [((n, D), BF, (n, D), lambda i: (0, 0)) for n in rows],
                 moved=4096 * sum(rows), flops=2**26)


def join_columns(g):
    return jnp.concatenate([g[j * UNIT : (j + 1) * UNIT, k * UNIT : (k + 1) * UNIT] for k in range(8) for j in range(3)], 1)


def solution(mesh):
    def step(x, dy, *arrays):
        weights, m, v = (arrays[i : i + 7] for i in (0, 7, 14))
        wq, wk, wv, wo, wg, wu, wd = weights
        x, dy = x[0], dy[0]
        t = x.shape[0]

        (p1,) = pack([(wq, 0), (wk, 0), (wv, 0)])
        p2, p3, p4 = pack([(wo, 0), (wg, 0), (wu, 0), (wd, 1)], [(wq, 1), (wk, 1), (wv, 1), (wd, 0)], [(wo, 1), (wg, 1), (wu, 1)])
        g1, g2, g3, g4 = (lax.all_gather(p, "dp", axis=0) for p in (p1, p2, p3, p4))

        angle = jnp.arange(t, dtype=F32)[:, None] * THETA ** (-jnp.arange(HEAD // 2, dtype=F32) / (HEAD // 2))
        cos, sin = jnp.cos(angle), jnp.sin(angle)
        cos, sin = jnp.concatenate([cos, cos], 1), jnp.concatenate([-sin, sin], 1)

        def scatter(units, after=None):
            if after is not None:
                units, _ = lax.optimization_barrier((units, after))
            return lax.psum_scatter(units.reshape(-1, D), "dp", scatter_dimension=0, tiled=True)

        a0, q0, k0, v0 = qkv(x, g1, 0, cos, sin)
        o0, lse0 = attend(q0, k0, v0)
        h1, b0 = out_proj(x, o0, g2, 0)
        gate, up, act0 = ffn_up(b0, g2, 1, 4)
        d1, act0 = lax.optimization_barrier((ffn_mid(dy, g2, 7), act0))
        h2 = ffn_down(h1, act0, g3, 3)
        a1, q1, k1, v1 = qkv(h2, g3, 0, cos, sin)
        o1, lse1 = attend(q1, k1, v1)
        h3, b1 = out_proj(h2, o1, g4, 0)
        act1, dg1, du1 = ffn_last(b1, d1, g4, 1, 4)

        def ffn_grads(b, dg, du, act, dh):
            return weight_grads([*(((b, 0), (dg, j)) for j in range(3)), *(((b, 0), (du, j)) for j in range(3)),
                                 *(((act, j), (dh, 0)) for j in range(3))])

        def attention_grads(a, dq, dk, dv, o, dh):
            return weight_grads([((a, 0), (dq, 0)), ((a, 0), (dk, 0)), ((a, 0), (dv, 0)), ((o, 0), (dh, 0))])

        f1, dg1, du1 = lax.optimization_barrier((ffn_grads(b1, dg1, du1, act1, dy), dg1, du1))
        rf1 = scatter(f1)
        dh3, do1 = ffn_in_bwd(dg1, du1, g4, 1, 4, g4, 0, h3, dy)
        dq1, dk1, dv1 = attend_bwd(q1, k1, v1, do1, o1, lse1, cos, sin)
        t1, dq1, dk1, dv1 = lax.optimization_barrier((attention_grads(a1, dq1, dk1, dv1, o1, dh3), dq1, dk1, dv1))
        rt1 = scatter(t1, rf1)
        dh2 = qkv_bwd(dq1, dk1, dv1, g3, 0, h2, dh3)
        dg0, du0 = ffn_act_bwd(dh2, gate, up, g3, 3)
        f0, dg0, du0 = lax.optimization_barrier((ffn_grads(b0, dg0, du0, act0, dh2), dg0, du0))
        rf0 = scatter(f0, rt1)
        dh1, do0 = ffn_in_bwd(dg0, du0, g2, 1, 4, g2, 0, h1, dh2)
        dq0, dk0, dv0 = attend_bwd(q0, k0, v0, do0, o0, lse0, cos, sin)
        rt0 = scatter(attention_grads(a0, dq0, dk0, dv0, o0, dh1), rf0)

        def blocks(f, a):
            return [*jnp.split(a, 4), *map(join_columns, jnp.split(f, 3)[:2]), jnp.split(f, 3)[2]]

        squares = total_squares(sum(jnp.sum(jnp.square(r.astype(F32))) for r in (rf1, rt1, rf0)), rt0, mesh.shape["dp"])
        gradients = [jnp.stack(pair).astype(F32) for pair in zip(blocks(rf0, rt0), blocks(rf1, rt1), strict=True)]
        gradients = clipped(gradients, squares, lax.psum(1, "dp") * sum(g.size for g in gradients))
        new = [adamw(w.astype(F32), m, v, g) for w, m, v, g in zip(weights, m, v, gradients, strict=True)]
        return tuple(one[which] for which in range(3) for one in new)

    states, cut = P(("rep", "dp"), None, None), P(None, "dp", None)
    return jax.shard_map(
        step,
        mesh=mesh,
        in_specs=(states, states) + (cut,) * 21,
        out_specs=(P("rep", "dp", None),) * 21,
        check_vma=False,
    )
```
